32 devices in a mesh: samp: 8 (over y, x, core), snp: 4 (over z).
Axes of the slice: x: 2, y: 2, z: 4, core: 2. Of those that a mesh axis runs over, the one named last changes fastest.
Arguments:
- genotypes: bfloat16 [8192, 16384], P('samp', 'snp'), may hold values from -6 to 6
- probes: bfloat16 [8, 8192], P(None, 'samp'), may hold values from -6 to 6
- env_label: int32 [8192], P('samp'), may hold values from 0 to 7
- variances: float32 [3], replicated, may hold values from 0.25 to 1
Outputs:
- first: float32 [8, 8192], P(None, 'samp')
- second: float32 [8, 8192], P(None, 'samp')
The draws below stay inside these ranges and needn't reach their ends.
All inputs are finite; a program needn't handle non-finite values.
Results may differ from the reference program's by a relative error of at most 0.0018.
Values may be sent and summed in bfloat16 or wider, within the bound.
A program may use at most 64 MiB of HBM per device.

```python
import math
import jax
import jax.numpy as jnp
from jax import lax

SNPS = 16384
PROBES = 8
ENVS = 8
SAMPLES = 8192


def place_ends(drawn, key, low, largest):
    place = [jax.random.randint(jax.random.fold_in(key, axis), (), 0, length) for axis, length in enumerate(drawn.shape)]
    widest = drawn.shape.index(max(drawn.shape))
    neighbour = place[:widest] + [(place[widest] + 1) % drawn.shape[widest]] + place[widest + 1:]
    return drawn.at[tuple(place)].set(low).at[tuple(neighbour)].set(largest)


def block_scale(stream_key, shape, cuts, low, largest):
    def one(dim, shards_of):
        draws = jax.random.uniform(jax.random.fold_in(jax.random.fold_in(stream_key, 6), dim), (shards_of,), jnp.float32, low / len(cuts), largest / len(cuts))
        return jnp.repeat(jnp.exp(draws), shape[dim] // shards_of).reshape((-1,) + (1,) * (len(shape) - dim - 1))

    factor_of = one(*cuts[0])
    for cut in cuts[1:]:
        factor_of = factor_of * one(*cut)
    return factor_of


def centred(key, shape, spread, bound, split=(), kind=jnp.bfloat16):
    gain = block_scale(key, shape, split, -0.22, 0.18) if split else 1.0
    result = jax.random.normal(key, shape, jnp.float32) * spread * gain
    return jnp.minimum(jnp.maximum(result, -bound), bound).astype(kind)


def setup_inputs(seed: int = 0) -> dict:
    streams_of = jax.random.split(jax.random.key(seed), 5)
    return {
        "genotypes": centred(streams_of[0], (SAMPLES, SNPS), 1.0, 6.0, ((0, 8), (1, 4))),
        "probes": centred(streams_of[1], (PROBES, SAMPLES), 1.0, 6.0, ((1, 8),)),
        "env_label": place_ends(jax.random.randint(streams_of[2], (SAMPLES,), 0, ENVS), jax.random.fold_in(streams_of[2], 1), 0, ENVS - 1).astype(jnp.int32),
        "variances": jnp.clip(jnp.exp(jax.random.uniform(streams_of[3], (3,), jnp.float32, math.log(0.25), math.log(1.0))), 0.25, 1.0),
    }


def apply_operator(current, genotypes, onehot, variances):
    rounded = current.astype(jnp.bfloat16)
    scaled = (onehot[:, None, :] * rounded[None, :, :]).reshape(ENVS * PROBES, -1)
    panel = jnp.concatenate([rounded, scaled], axis=0)
    snp_panel = jnp.dot(panel, genotypes, preferred_element_type=jnp.float32).astype(jnp.bfloat16)
    image = lax.dot_general(snp_panel, genotypes, (((1,), (1,)), ((), ())), preferred_element_type=jnp.float32)
    additive = image[:PROBES]
    blocks = image[PROBES:].reshape(ENVS, PROBES, -1)
    interaction = jnp.sum(onehot.astype(jnp.float32)[:, None, :] * blocks, axis=0)
    return variances[0] * additive / SNPS + variances[1] * interaction / SNPS + variances[2] * current


def reference(genotypes, probes, env_label, variances):
    labels = jnp.arange(ENVS, dtype=jnp.int32)
    onehot = (env_label[None, :] == labels[:, None]).astype(jnp.bfloat16)
    first = apply_operator(probes.astype(jnp.float32), genotypes, onehot, variances)
    second = apply_operator(first, genotypes, onehot, variances)
    return first, second
```

```python
import functools

import jax
import jax.numpy as jnp
from jax import lax
from jax.experimental import pallas as pl
from jax.experimental.pallas import tpu as pltpu
from jax.sharding import PartitionSpec as P

ENVS = 8


def plan(samp, cols):
    chips = samp // 2
    share = cols // samp
    stages = 2 if share % 256 == 0 else 1
    return chips, share, stages, share // stages


def kernel(
    samp, snp, z_hbm, probes_ref, label_ref, var_ref, first_ref, second_ref,
    z, panel, onehot, mine, pair_out, pair_in, rs_out, rs_in, ag, image, weighted, z_in,
    load_sem, pair_s, pair_r, rs_s, rs_r, ag_s, ag_r, fw_s, fw_r, zs_s, zs_r,
):
    probes, local = probes_ref.shape
    cols = z.shape[1]
    rows = ENVS * probes
    chips, share, stages, sub = plan(samp, cols)
    me = lax.axis_index("samp")
    chip, core = me // 2, me % 2
    here = lax.axis_index("snp")

    def device(other_chip, other_core):
        return {"samp": other_chip * 2 + other_core}

    def ahead(r):
        return lax.rem(chip + r, chips)

    def behind(r):
        return lax.rem(chip - r + chips, chips)

    def start_of(which_core, which_chip, j):
        return pl.multiple_of((which_core * chips + which_chip) * share + j * sub, 128)

    def load(j, away, k):
        side = (1 - core) if away else core
        at = pl.ds(start_of(side, k, j), sub)
        return pltpu.make_async_copy(z_hbm.at[:, at], z.at[:, at], load_sem.at[j, int(away), k])

    for j in range(stages):
        for away in (True, False):
            for k in range(chips):
                load(j, away, k).start()

    barrier = pltpu.get_barrier_semaphore()
    peers = [device(chip, 1 - core)]
    peers += [device(ahead(r), core) for r in range(1, chips)]
    peers += [{"snp": lax.rem(here + r, snp)} for r in range(1, snp)]
    for peer in peers:
        pl.semaphore_signal(barrier, inc=1, device_id=peer, device_id_type=pl.DeviceIdType.MESH)

    labels = label_ref[...]
    for e in range(ENVS):
        onehot[e * probes:(e + 1) * probes, :] = jnp.broadcast_to(
            (labels == e).astype(jnp.float32), (probes, local))

    def remote(src, dst, send, recv, to):
        return pltpu.make_async_remote_copy(
            src_ref=src, dst_ref=dst, send_sem=send, recv_sem=recv,
            device_id=to, device_id_type=pl.DeviceIdType.MESH)

    sent = []
    for op in range(2):
        current = probes_ref[...].astype(jnp.float32) if op == 0 else first_ref[...]
        rounded = current.astype(jnp.bfloat16).astype(jnp.float32)
        for e in range(ENVS):
            block = slice(e * probes, (e + 1) * probes)
            panel[block, :] = (onehot[block, :] * rounded).astype(jnp.bfloat16)

        def matmul(away, j, k):
            side = (1 - core) if away else core
            if op == 0:
                load(j, away, k).wait()
            return jnp.dot(panel[...], z[:, pl.ds(start_of(side, k, j), sub)], preferred_element_type=jnp.float32)

        def pair(j):
            return remote(pair_out.at[op, j], pair_in.at[op, j], pair_s.at[op, j], pair_r.at[op, j],
                          device(chip, 1 - core))

        def scatter(j, r):
            return remote(rs_out.at[op, j, r], rs_in.at[op, j, r], rs_s.at[op, j, r], rs_r.at[op, j, r],
                          device(ahead(r), core))

        def gather(j, r):
            at = ag.at[op, j, core, chip]
            return remote(at, at, ag_s.at[op, j, r], ag_r.at[op, j, r], device(ahead(r), core))

        def forward(j, r):
            at = ag.at[op, j, core, behind(r)]
            return remote(at, at, fw_s.at[op, j, r], fw_r.at[op, j, r], device(chip, 1 - core))

        def send(copy):
            copy.start()
            sent.append(copy)

        def away_part(j):
            def body(k, _):
                pair_out[op, j, k] = matmul(True, j, k)
                return 0
            lax.fori_loop(0, chips, body, 0)
            if op == 0 and j == 0:
                pl.semaphore_wait(barrier, len(peers))
            send(pair(j))

        def own_part(j):
            def body(k, _):
                mine[j, k] = matmul(False, j, k)
                return 0
            lax.fori_loop(0, chips, body, 0)

        def reduce_pair(j):
            pair(j).wait_recv()
            for r in range(1, chips):
                k = ahead(r)
                rs_out[op, j, r] = mine[j, k] + pair_in[op, j, k]
                send(scatter(j, r))

        def finish_panel(j):
            total = mine[j, chip] + pair_in[op, j, chip]
            for r in range(1, chips):
                scatter(j, r).wait_recv()
                total = total + rs_in[op, j, r]
            plain = total[:probes]
            for e in range(1, ENVS):
                plain = plain + total[e * probes:(e + 1) * probes]
            ag[op, j, core, chip] = jnp.concatenate([plain, total], axis=0).astype(jnp.bfloat16)
            for r in range(1, chips):
                send(gather(j, r))
            send(forward(j, 0))

        def add_image(j, which_core, which_chip):
            part = lax.dot_general(
                ag[op, j, which_core, which_chip], z[:, pl.ds(start_of(which_core, which_chip, j), sub)],
                (((1,), (1,)), ((), ())), preferred_element_type=jnp.float32)
            image[...] += part

        away_part(0)
        own_part(0)
        for j in range(1, stages):
            away_part(j)
            reduce_pair(j - 1)
            own_part(j)
        reduce_pair(stages - 1)
        image[...] = jnp.zeros_like(image)
        for j in range(stages):
            finish_panel(j)
        for j in range(stages):
            add_image(j, core, chip)
        for j in range(stages):
            for r in range(1, chips):
                gather(j, r).wait_recv()
                send(forward(j, r))
                add_image(j, core, behind(r))
            for r in range(chips):
                forward(j, r).wait_recv()
                add_image(j, 1 - core, behind(r))

        total_snps = cols * snp
        interaction = jnp.zeros((probes, local), jnp.float32)
        for e in range(ENVS):
            block = slice(e * probes, (e + 1) * probes)
            interaction = interaction + onehot[block, :] * image[probes + e * probes:probes + (e + 1) * probes, :]
        weighted[op] = var_ref[0] * image[:probes, :] / total_snps + var_ref[1] * interaction / total_snps

        def over_snps(r):
            return remote(weighted.at[op], z_in.at[op, r], zs_s.at[op, r], zs_r.at[op, r],
                          {"snp": lax.rem(here + r, snp)})

        for r in range(1, snp):
            send(over_snps(r))
        for r in range(1, snp):
            over_snps(r).wait_recv()
        parts = [weighted[op]] + [z_in[op, r] for r in range(1, snp)]
        total = jnp.zeros((probes, local), jnp.float32)
        for s in range(snp):
            term = parts[0]
            for r in range(1, snp):
                term = jnp.where(lax.rem(here - r + snp, snp) == s, parts[r], term)
            total = total + term
        out = first_ref if op == 0 else second_ref
        out[...] = total + var_ref[2] * current
    for copy in sent:
        copy.wait_send()


def solution(mesh):
    samp, snp = mesh.shape["samp"], mesh.shape["snp"]

    def per_device(genotypes, probes, env_label, variances):
        local, cols = genotypes.shape
        count = probes.shape[0]
        rows = ENVS * count
        chips, _, stages, sub = plan(samp, cols)
        vmem = pltpu.VMEM
        dma = pltpu.SemaphoreType.DMA
        out = jax.ShapeDtypeStruct((count, local), jnp.float32)
        whole = pl.BlockSpec(memory_space=pltpu.VMEM)
        return pl.pallas_call(
            functools.partial(kernel, samp, snp),
            out_shape=(out, out),
            in_specs=[pl.BlockSpec(memory_space=pl.ANY), whole, whole, pl.BlockSpec(memory_space=pltpu.SMEM)],
            out_specs=(whole, whole),
            scratch_shapes=[
                vmem((local, cols), jnp.bfloat16),
                vmem((rows, local), jnp.bfloat16),
                vmem((rows, local), jnp.float32),
                vmem((stages, chips, rows, sub), jnp.float32),
                vmem((2, stages, chips, rows, sub), jnp.float32),
                vmem((2, stages, chips, rows, sub), jnp.float32),
                vmem((2, stages, chips, rows, sub), jnp.float32),
                vmem((2, stages, chips, rows, sub), jnp.float32),
                vmem((2, stages, 2, chips, rows + count, sub), jnp.bfloat16),
                vmem((rows + count, local), jnp.float32),
                vmem((2, count, local), jnp.float32),
                vmem((2, snp, count, local), jnp.float32),
                dma((stages, 2, chips)),
                dma((2, stages)), dma((2, stages)),
                dma((2, stages, chips)), dma((2, stages, chips)),
                dma((2, stages, chips)), dma((2, stages, chips)),
                dma((2, stages, chips)), dma((2, stages, chips)),
                dma((2, snp)), dma((2, snp)),
            ],
            compiler_params=pltpu.CompilerParams(
                collective_id=0, has_side_effects=True, vmem_limit_bytes=56 * 1024 * 1024),
        )(genotypes, probes, env_label.reshape(1, local), variances)

    return jax.shard_map(
        per_device,
        mesh=mesh,
        in_specs=(P("samp", "snp"), P(None, "samp"), P("samp"), P()),
        out_specs=(P(None, "samp"), P(None, "samp")),
        check_vma=False,
    )
```

```python
import functools

import jax
import jax.numpy as jnp
from jax import lax
from jax.experimental import pallas as pl
from jax.experimental.pallas import tpu as pltpu
from jax.sharding import PartitionSpec as P

ENVS = 8


def plan(samp, cols):
    chips = samp // 2
    share = cols // samp
    stages = 2 if share % 256 == 0 else 1
    return chips, share, stages, share // stages


def kernel(
    samp, snp, z_hbm, probes_ref, label_ref, var_ref, first_ref, second_ref,
    z, panel, onehot, mine, pair_out, pair_in, rs_out, rs_in, ag, image, z_in,
    load_sem, pair_s, pair_r, rs_s, rs_r, ag_s, ag_r, fw_s, fw_r, zs_s, zs_r,
):
    probes, local = probes_ref.shape
    cols = z.shape[1]
    rows = ENVS * probes
    chips, share, stages, sub = plan(samp, cols)
    me = lax.axis_index("samp")
    chip, core = me // 2, me % 2
    here = lax.axis_index("snp")

    def device(other_chip, other_core):
        return {"samp": other_chip * 2 + other_core}

    def partner(r):
        if chips & (chips - 1):
            return lax.rem(chip + r, chips)
        return sum(lax.rem(chip // bit + r // bit, 2) * bit for bit in (1 << b for b in range(chips.bit_length() - 1)))

    def source(r):
        return lax.rem(chip - r + chips, chips) if chips & (chips - 1) else partner(r)

    width = chips * sub

    def start_of(which_core, j):
        return pl.multiple_of(which_core * (cols // 2) + j * width, 128)

    def columns(which_chip):
        return pl.ds(pl.multiple_of(which_chip * sub, 128), sub)

    def load(j, away):
        at = pl.ds(start_of((1 - core) if away else core, j), width)
        return pltpu.make_async_copy(z_hbm.at[:, at], z.at[:, at], load_sem.at[j, int(away)])

    for j in range(stages):
        for away in (True, False):
            load(j, away).start()

    barrier = pltpu.get_barrier_semaphore()
    peers = [device(chip, 1 - core)]
    peers += [device(partner(r), core) for r in range(1, chips)]
    peers += [{"snp": lax.rem(here + r, snp)} for r in range(1, snp)]
    for peer in peers:
        pl.semaphore_signal(barrier, inc=1, device_id=peer, device_id_type=pl.DeviceIdType.MESH)

    labels = label_ref[...]
    for e in range(ENVS):
        onehot[e * probes:(e + 1) * probes, :] = jnp.broadcast_to(
            (labels == e).astype(jnp.float32), (probes, local))

    def remote(src, dst, send, recv, to):
        return pltpu.make_async_remote_copy(
            src_ref=src, dst_ref=dst, send_sem=send, recv_sem=recv,
            device_id=to, device_id_type=pl.DeviceIdType.MESH)

    def sum_blocks(blocks):
        total = blocks[:probes]
        for e in range(1, ENVS):
            total = total + blocks[e * probes:(e + 1) * probes]
        return total

    sent = []
    for op in range(2):
        current = probes_ref[...].astype(jnp.float32) if op == 0 else first_ref[...]
        rounded = current.astype(jnp.bfloat16).astype(jnp.float32)
        for e in range(ENVS):
            block = slice(e * probes, (e + 1) * probes)
            panel[block, :] = (onehot[block, :] * rounded).astype(jnp.bfloat16)

        def matmul(away, j):
            if op == 0:
                load(j, away).wait()
            at = pl.ds(start_of((1 - core) if away else core, j), width)
            return jnp.dot(panel[...], z[:, at], preferred_element_type=jnp.float32)

        def pair(j):
            return remote(pair_out.at[op, j], pair_in.at[op, j], pair_s.at[op, j], pair_r.at[op, j],
                          device(chip, 1 - core))

        def scatter(j, r):
            return remote(rs_out.at[op, j, r], rs_in.at[op, j, r], rs_s.at[op, j, r], rs_r.at[op, j, r],
                          device(partner(r), core))

        def gather(j, r):
            at = ag.at[op, j, core, chip]
            return remote(at, at, ag_s.at[op, j, r], ag_r.at[op, j, r], device(partner(r), core))

        def forward(j, r):
            at = ag.at[op, j, core, source(r)]
            return remote(at, at, fw_s.at[op, j, r], fw_r.at[op, j, r], device(chip, 1 - core))

        def send(copy):
            copy.start()
            sent.append(copy)

        def away_part(j):
            pair_out[op, j] = matmul(True, j)

        def own_part(j):
            mine[j] = matmul(False, j)

        def reduce_pair(j):
            pair(j).wait_recv()
            for r in reversed(range(1, chips)):
                at = columns(partner(r))
                both = mine[j, :, at] + pair_in[op, j, :, at]
                short = both.astype(jnp.bfloat16)
                rest = both - short.astype(jnp.float32)
                lost = sum_blocks(rest).astype(jnp.bfloat16)
                rs_out[op, j, r] = jnp.concatenate([lost, short], axis=0)
                send(scatter(j, r))

        def finish_panel(j):
            at = columns(chip)
            total = mine[j, :, at] + pair_in[op, j, :, at]
            lost = jnp.zeros((probes, sub), jnp.float32)
            for r in range(1, chips):
                scatter(j, r).wait_recv()
                came = rs_in[op, j, r].astype(jnp.float32)
                total = total + came[probes:]
                lost = lost + came[:probes]
            plain = sum_blocks(total) + lost
            ag[op, j, core, chip] = jnp.concatenate([plain, total], axis=0).astype(jnp.bfloat16)
            for r in reversed(range(1, chips)):
                send(gather(j, r))
            send(forward(j, 0))

        def add_image(j, which_core, which_chip):
            at = pl.ds(pl.multiple_of(start_of(which_core, j) + which_chip * sub, 128), sub)
            part = lax.dot_general(
                ag[op, j, which_core, which_chip], z[:, at],
                (((1,), (1,)), ((), ())), preferred_element_type=jnp.float32)
            image[...] += part

        away_part(0)
        if op == 0:
            own_part(0)
            pl.semaphore_wait(barrier, len(peers))
        send(pair(0))
        if op == 1:
            own_part(0)
        for j in range(1, stages):
            away_part(j)
            send(pair(j))
            reduce_pair(j - 1)
            own_part(j)
        reduce_pair(stages - 1)
        image[...] = jnp.zeros_like(image)
        for j in range(stages):
            finish_panel(j)
        for j in range(stages):
            add_image(j, core, chip)
        for j in range(stages):
            for r in range(1, chips):
                gather(j, r).wait_recv()
                send(forward(j, r))
                add_image(j, core, source(r))
            for r in range(chips):
                forward(j, r).wait_recv()
                add_image(j, 1 - core, source(r))

        total_snps = cols * snp
        interaction = jnp.zeros((probes, local), jnp.float32)
        for e in range(ENVS):
            block = slice(e * probes, (e + 1) * probes)
            interaction = interaction + onehot[block, :] * image[probes + e * probes:probes + (e + 1) * probes, :]
        z_in[op, here] = var_ref[0] * image[:probes, :] / total_snps + var_ref[1] * interaction / total_snps

        def other_snp(r):
            return lax.rem(here + jnp.where(here < snp // 2, snp - r, r), snp)

        def over_snps(r, recv):
            return remote(z_in.at[op, here], z_in.at[op, here], zs_s.at[op, r], zs_r.at[op, recv],
                          {"snp": other_snp(r)})

        for r in range(1, snp):
            send(over_snps(r, here))
        for r in range(1, snp):
            over_snps(r, other_snp(r)).wait_recv()
        total = z_in[op, 0]
        for s in range(1, snp):
            total = total + z_in[op, s]
        out = first_ref if op == 0 else second_ref
        out[...] = total + var_ref[2] * current
    for copy in sent:
        copy.wait_send()


def solution(mesh):
    samp, snp = mesh.shape["samp"], mesh.shape["snp"]

    def per_device(genotypes, probes, env_label, variances):
        local, cols = genotypes.shape
        count = probes.shape[0]
        rows = ENVS * count
        chips, _, stages, sub = plan(samp, cols)
        vmem = pltpu.VMEM
        dma = pltpu.SemaphoreType.DMA
        out = jax.ShapeDtypeStruct((count, local), jnp.float32)
        whole = pl.BlockSpec(memory_space=pltpu.VMEM)
        return pl.pallas_call(
            functools.partial(kernel, samp, snp),
            out_shape=(out, out),
            in_specs=[pl.BlockSpec(memory_space=pl.ANY), whole, whole, pl.BlockSpec(memory_space=pltpu.SMEM)],
            out_specs=(whole, whole),
            scratch_shapes=[
                vmem((local, cols), jnp.bfloat16),
                vmem((rows, local), jnp.bfloat16),
                vmem((rows, local), jnp.float32),
                vmem((stages, rows, chips * sub), jnp.float32),
                vmem((2, stages, rows, chips * sub), jnp.float32),
                vmem((2, stages, rows, chips * sub), jnp.float32),
                vmem((2, stages, chips, rows + count, sub), jnp.bfloat16),
                vmem((2, stages, chips, rows + count, sub), jnp.bfloat16),
                vmem((2, stages, 2, chips, rows + count, sub), jnp.bfloat16),
                vmem((rows + count, local), jnp.float32),
                vmem((2, snp, count, local), jnp.float32),
                dma((stages, 2)),
                dma((2, stages)), dma((2, stages)),
                dma((2, stages, chips)), dma((2, stages, chips)),
                dma((2, stages, chips)), dma((2, stages, chips)),
                dma((2, stages, chips)), dma((2, stages, chips)),
                dma((2, snp)), dma((2, snp)),
            ],
            compiler_params=pltpu.CompilerParams(
                collective_id=0, has_side_effects=True, vmem_limit_bytes=56 * 1024 * 1024),
        )(genotypes, probes, env_label.reshape(1, local), variances)

    return jax.shard_map(
        per_device,
        mesh=mesh,
        in_specs=(P("samp", "snp"), P(None, "samp"), P("samp"), P()),
        out_specs=(P(None, "samp"), P(None, "samp")),
        check_vma=False,
    )
```

```python
import functools

import jax
import jax.numpy as jnp
from jax import lax
from jax.experimental import pallas as pl
from jax.experimental.pallas import tpu as pltpu
from jax.sharding import PartitionSpec as P

ENVS = 8


def plan(samp, cols):
    chips = samp // 2
    share = cols // samp
    stages = 2 if share % 256 == 0 else 1
    return chips, share, stages, share // stages


def kernel(
    samp, snp, z_hbm, probes_hbm, label_hbm, var_ref, first_ref, second_ref,
    z, probes_ref, label_ref, panel, onehot, mine, pair_out, pair_in, rs_out, rs_in, ag, image, z_in,
    load_sem, small_sem, pair_s, pair_r, rs_s, rs_r, ag_s, ag_r, fw_s, fw_r, zs_s, zs_r,
):
    probes, local = probes_hbm.shape
    cols = z.shape[1]
    rows = ENVS * probes
    chips, share, stages, sub = plan(samp, cols)
    me = lax.axis_index("samp")
    chip, core = me // 2, me % 2
    here = lax.axis_index("snp")

    def device(other_chip, other_core):
        return {"samp": other_chip * 2 + other_core}

    def partner(r):
        if chips & (chips - 1):
            return lax.rem(chip + r, chips)
        return sum(lax.rem(chip // bit + r // bit, 2) * bit for bit in (1 << b for b in range(chips.bit_length() - 1)))

    def source(r):
        return lax.rem(chip - r + chips, chips) if chips & (chips - 1) else partner(r)

    width = chips * sub

    def start_of(which_core, j):
        return pl.multiple_of(which_core * (cols // 2) + j * width, 128)

    order = list(reversed(range(chips)))

    def load(j, away):
        at = pl.ds(start_of((1 - core) if away else core, j), width)
        return pltpu.make_async_copy(z_hbm.at[:, at], z.at[:, at], load_sem.at[j, int(away)])

    small = [pltpu.make_async_copy(label_hbm, label_ref, small_sem.at[0]),
             pltpu.make_async_copy(probes_hbm, probes_ref, small_sem.at[1])]
    for copy in small:
        copy.start()
    for j in range(stages):
        for away in (True, False):
            load(j, away).start()

    barrier = pltpu.get_barrier_semaphore()
    peers = [device(chip, 1 - core)]
    peers += [device(partner(r), core) for r in range(1, chips)]
    peers += [{"snp": lax.rem(here + r, snp)} for r in range(1, snp)]
    for peer in peers:
        pl.semaphore_signal(barrier, inc=1, device_id=peer, device_id_type=pl.DeviceIdType.MESH)

    for copy in small:
        copy.wait()
    labels = label_ref[...]
    for e in range(ENVS):
        onehot[e * probes:(e + 1) * probes, :] = jnp.broadcast_to(
            (labels == e).astype(jnp.float32), (probes, local))

    def remote(src, dst, send, recv, to):
        return pltpu.make_async_remote_copy(
            src_ref=src, dst_ref=dst, send_sem=send, recv_sem=recv,
            device_id=to, device_id_type=pl.DeviceIdType.MESH)

    def sum_blocks(blocks):
        total = blocks[:probes]
        for e in range(1, ENVS):
            total = total + blocks[e * probes:(e + 1) * probes]
        return total

    sent = []
    for op in range(2):
        current = probes_ref[...].astype(jnp.float32) if op == 0 else first_ref[...]
        rounded = current.astype(jnp.bfloat16).astype(jnp.float32)
        for e in range(ENVS):
            block = slice(e * probes, (e + 1) * probes)
            panel[block, :] = (onehot[block, :] * rounded).astype(jnp.bfloat16)

        def matmul(away, j):
            if op == 0:
                load(j, away).wait()
            at = pl.ds(start_of((1 - core) if away else core, j), width)
            return jnp.dot(panel[...], z[:, at], preferred_element_type=jnp.float32)

        def pair(j, r):
            at = (op, j, partner(r))
            return remote(pair_out.at[at], pair_in.at[at], pair_s.at[op, j, r], pair_r.at[op, j, r],
                          device(chip, 1 - core))

        def scatter(j, r):
            return remote(rs_out.at[op, j, r], rs_in.at[op, j, r], rs_s.at[op, j, r], rs_r.at[op, j, r],
                          device(partner(r), core))

        def gather(j, r):
            at = ag.at[op, j, core, chip]
            return remote(at, at, ag_s.at[op, j, r], ag_r.at[op, j, r], device(partner(r), core))

        def forward(j, r):
            at = ag.at[op, j, core, source(r)]
            return remote(at, at, fw_s.at[op, j, r], fw_r.at[op, j, r], device(chip, 1 - core))

        def send(copy):
            copy.start()
            sent.append(copy)

        def away_part(j):
            part = matmul(True, j)
            for k in range(chips):
                pair_out[op, j, k] = part[:, k * sub:(k + 1) * sub]

        def send_pair(j):
            for r in order:
                send(pair(j, r))

        def own_part(j):
            part = matmul(False, j)
            for k in range(chips):
                mine[j, k] = part[:, k * sub:(k + 1) * sub]

        def reduce_pair(j):
            for r in order[:-1]:
                pair(j, r).wait_recv()
                both = mine[j, partner(r)] + pair_in[op, j, partner(r)]
                short = both.astype(jnp.bfloat16)
                rest = both - short.astype(jnp.float32)
                lost = sum_blocks(rest).astype(jnp.bfloat16)
                rs_out[op, j, r] = jnp.concatenate([lost, short], axis=0)
                send(scatter(j, r))

        def finish_panel(j):
            pair(j, 0).wait_recv()
            total = mine[j, chip] + pair_in[op, j, chip]
            lost = jnp.zeros((probes, sub), jnp.float32)
            for r in range(1, chips):
                scatter(j, r).wait_recv()
                came = rs_in[op, j, r].astype(jnp.float32)
                total = total + came[probes:]
                lost = lost + came[:probes]
            plain = sum_blocks(total) + lost
            ag[op, j, core, chip] = jnp.concatenate([plain, total], axis=0).astype(jnp.bfloat16)
            for r in reversed(range(1, chips)):
                send(gather(j, r))
            send(forward(j, 0))

        def add_image(j, which_core, which_chip):
            at = pl.ds(pl.multiple_of(start_of(which_core, j) + which_chip * sub, 128), sub)
            part = lax.dot_general(
                ag[op, j, which_core, which_chip], z[:, at],
                (((1,), (1,)), ((), ())), preferred_element_type=jnp.float32)
            image[...] += part

        away_part(0)
        if op == 0:
            own_part(0)
            pl.semaphore_wait(barrier, len(peers))
        send_pair(0)
        if op == 1:
            own_part(0)
        for j in range(1, stages):
            away_part(j)
            send_pair(j)
            reduce_pair(j - 1)
            own_part(j)
        reduce_pair(stages - 1)
        image[...] = jnp.zeros_like(image)
        for j in range(stages):
            finish_panel(j)
        for j in range(stages):
            add_image(j, core, chip)
        for j in range(stages):
            for r in range(1, chips):
                gather(j, r).wait_recv()
                send(forward(j, r))
                add_image(j, core, source(r))
            for r in range(chips):
                forward(j, r).wait_recv()
                add_image(j, 1 - core, source(r))

        total_snps = cols * snp
        interaction = jnp.zeros((probes, local), jnp.float32)
        for e in range(ENVS):
            block = slice(e * probes, (e + 1) * probes)
            interaction = interaction + onehot[block, :] * image[probes + e * probes:probes + (e + 1) * probes, :]
        z_in[op, here] = var_ref[0] * image[:probes, :] / total_snps + var_ref[1] * interaction / total_snps

        def other_snp(r):
            return lax.rem(here + jnp.where(here < snp // 2, snp - r, r), snp)

        def over_snps(r, recv):
            return remote(z_in.at[op, here], z_in.at[op, here], zs_s.at[op, r], zs_r.at[op, recv],
                          {"snp": other_snp(r)})

        for r in range(1, snp):
            send(over_snps(r, here))
        for r in range(1, snp):
            over_snps(r, other_snp(r)).wait_recv()
        total = z_in[op, 0]
        for s in range(1, snp):
            total = total + z_in[op, s]
        out = first_ref if op == 0 else second_ref
        out[...] = total + var_ref[2] * current
    for copy in sent:
        copy.wait_send()


def solution(mesh):
    samp, snp = mesh.shape["samp"], mesh.shape["snp"]

    def per_device(genotypes, probes, env_label, variances):
        local, cols = genotypes.shape
        count = probes.shape[0]
        rows = ENVS * count
        chips, _, stages, sub = plan(samp, cols)
        vmem = pltpu.VMEM
        dma = pltpu.SemaphoreType.DMA
        out = pltpu.VMEM((count, local), jnp.float32)
        anywhere = pl.BlockSpec(memory_space=pl.ANY)
        whole = pl.BlockSpec(memory_space=pltpu.VMEM)
        return pl.pallas_call(
            functools.partial(kernel, samp, snp),
            out_shape=(out, out),
            in_specs=[anywhere, anywhere, anywhere, pl.BlockSpec(memory_space=pltpu.SMEM)],
            out_specs=(whole, whole),
            scratch_shapes=[
                vmem((local, cols), jnp.bfloat16),
                vmem((count, local), jnp.bfloat16),
                vmem((1, local), jnp.int32),
                vmem((rows, local), jnp.bfloat16),
                vmem((rows, local), jnp.float32),
                vmem((stages, chips, rows, sub), jnp.float32),
                vmem((2, stages, chips, rows, sub), jnp.float32),
                vmem((2, stages, chips, rows, sub), jnp.float32),
                vmem((2, stages, chips, rows + count, sub), jnp.bfloat16),
                vmem((2, stages, chips, rows + count, sub), jnp.bfloat16),
                vmem((2, stages, 2, chips, rows + count, sub), jnp.bfloat16),
                vmem((rows + count, local), jnp.float32),
                vmem((2, snp, count, local), jnp.float32),
                dma((stages, 2)), dma((2,)),
                dma((2, stages, chips)), dma((2, stages, chips)),
                dma((2, stages, chips)), dma((2, stages, chips)),
                dma((2, stages, chips)), dma((2, stages, chips)),
                dma((2, stages, chips)), dma((2, stages, chips)),
                dma((2, snp)), dma((2, snp)),
            ],
            compiler_params=pltpu.CompilerParams(
                collective_id=0, has_side_effects=True, vmem_limit_bytes=56 * 1024 * 1024),
        )(genotypes, probes, env_label.reshape(1, local), variances)

    return jax.shard_map(
        per_device,
        mesh=mesh,
        in_specs=(P("samp", "snp"), P(None, "samp"), P("samp"), P()),
        out_specs=(P(None, "samp"), P(None, "samp")),
        check_vma=False,
    )
```

```python
import functools

import jax
import jax.numpy as jnp
from jax import lax
from jax.experimental import pallas as pl
from jax.experimental.pallas import tpu as pltpu
from jax.sharding import PartitionSpec as P

ENVS = 8
OPERATOR = (0, 1, 1, 0, 1, 0, 0, 1, 1)
TURNS = (0,) + OPERATOR + (0,) + OPERATOR + (0, 1)


def plan(samp, cols):
    chips = samp // 2
    share = cols // samp
    stages = 1
    return chips, share, stages, share // stages


def kernel(
    samp, snp, z_hbm, probes_hbm, label_hbm, var_ref, first_ref, second_ref,
    z, probes_ref, label_ref, panel, onehot, state, image, mine, pair_out, pair_in, rs_out, rs_in, ag, z_in,
    load_sem, small_sem, pair_s, pair_r, rs_s, rs_r, ag_s, ag_r, fw_s, fw_r, zs_s, zs_r,
):
    probes, local = probes_hbm.shape
    cols = z.shape[1]
    rows = ENVS * probes // 2
    half = local // 2
    chips, share, stages, sub = plan(samp, cols)
    me = lax.axis_index("samp")
    chip, core = me // 2, me % 2
    here = lax.axis_index("snp")

    def device(other_chip, other_core):
        return {"samp": other_chip * 2 + other_core}

    def partner(r):
        if chips & (chips - 1):
            return lax.rem(chip + r, chips)
        return sum(lax.rem(chip // bit + r // bit, 2) * bit for bit in (1 << b for b in range(chips.bit_length() - 1)))

    def source(r):
        return lax.rem(chip - r + chips, chips) if chips & (chips - 1) else partner(r)

    width = chips * sub

    def start_of(which_core, j):
        return pl.multiple_of(which_core * (cols // 2) + j * width, 128)

    order = list(reversed(range(chips)))

    def load(j, away):
        at = pl.ds(start_of((1 - core) if away else core, j), width)
        return pltpu.make_async_copy(z_hbm.at[:, at], z.at[:, at], load_sem.at[j, int(away)])

    small = [pltpu.make_async_copy(label_hbm, label_ref, small_sem.at[0]),
             pltpu.make_async_copy(probes_hbm, probes_ref, small_sem.at[1])]
    for copy in small:
        copy.start()
    for j in range(stages):
        for away in (True, False):
            load(j, away).start()

    barrier = pltpu.get_barrier_semaphore()
    peers = [device(chip, 1 - core)]
    peers += [device(partner(r), core) for r in range(1, chips)]
    peers += [{"snp": lax.rem(here + r, snp)} for r in range(1, snp)]
    for peer in peers:
        pl.semaphore_signal(barrier, inc=1, device_id=peer, device_id_type=pl.DeviceIdType.MESH)

    for copy in small:
        copy.wait()
    labels = label_ref[...]
    upper = lax.broadcasted_iota(jnp.int32, (probes, local), 0) < probes // 2
    packed_upper = lax.broadcasted_iota(jnp.int32, (probes, half), 0) < probes // 2

    def swap(tile):
        return pltpu.roll(tile, probes // 2, 0)

    tiles = [slice(i * probes, (i + 1) * probes) for i in range(ENVS // 2)]
    for i, tile in enumerate(tiles):
        onehot[tile, :] = (jnp.broadcast_to(labels, (probes, local)) == jnp.where(upper, 2 * i, 2 * i + 1)).astype(jnp.float32)

    def remote(src, dst, send, recv, to):
        return pltpu.make_async_remote_copy(
            src_ref=src, dst_ref=dst, send_sem=send, recv_sem=recv,
            device_id=to, device_id_type=pl.DeviceIdType.MESH)

    def sum_blocks(blocks):
        total = blocks[tiles[0]]
        for tile in tiles[1:]:
            total = total + blocks[tile]
        return total + swap(total)

    sent = []

    def send(copy):
        copy.start()
        sent.append(copy)

    def chain(group):
        everything = probes_ref[...].astype(jnp.float32)
        turned = swap(everything)
        state[group] = jnp.where(upper, everything, turned) if group == 0 else jnp.where(upper, turned, everything)
        for op in range(2):
            yield from operator(group, op)

    def operator(group, op):
        first_use = group == 0 and op == 0
        loads = op == 0 and group == 0
        t = group * 2 + op
        current = state[group]
        rounded = current.astype(jnp.bfloat16).astype(jnp.float32)
        panel[group] = jnp.concatenate([onehot[tile, :] * rounded for tile in tiles], axis=0).astype(jnp.bfloat16)

        def matmul(away, j):
            if loads:
                load(j, away).wait()
            at = pl.ds(start_of((1 - core) if away else core, j), width)
            return jnp.dot(panel[group], z[:, at], preferred_element_type=jnp.float32)

        def pair(j, r):
            at = (t, j, partner(r))
            return remote(pair_out.at[at], pair_in.at[at], pair_s.at[t, j, r], pair_r.at[t, j, r],
                          device(chip, 1 - core))

        def scatter(j, r):
            return remote(rs_out.at[t, j, r], rs_in.at[t, j, r], rs_s.at[t, j, r], rs_r.at[t, j, r],
                          device(partner(r), core))

        def gather(j, r):
            at = ag.at[t, j, core, chip]
            return remote(at, at, ag_s.at[t, j, r], ag_r.at[t, j, r], device(partner(r), core))

        def forward(j, r):
            at = ag.at[t, j, core, source(r)]
            return remote(at, at, fw_s.at[t, j, r], fw_r.at[t, j, r], device(chip, 1 - core))

        def away_part(j):
            part = matmul(True, j)
            for k in range(chips):
                pair_out[t, j, k] = part[:, k * sub:(k + 1) * sub]

        def send_pair(j):
            for r in order:
                send(pair(j, r))

        def own_part(j):
            part = matmul(False, j)
            for k in range(chips):
                mine[group, k] = part[:, k * sub:(k + 1) * sub]

        def reduce_pair(j):
            for r in order[:-1]:
                pair(j, r).wait_recv()
                both = mine[group, partner(r)] + pair_in[t, j, partner(r)]
                short = both.astype(jnp.bfloat16)
                rest = both - short.astype(jnp.float32)
                lost = sum_blocks(rest).astype(jnp.bfloat16)
                rs_out[t, j, r] = jnp.concatenate([lost, short], axis=0)
                send(scatter(j, r))

        def finish_panel(j):
            pair(j, 0).wait_recv()
            total = mine[group, chip] + pair_in[t, j, chip]
            lost = jnp.zeros((probes, sub), jnp.float32)
            for r in range(1, chips):
                scatter(j, r).wait_recv()
                came = rs_in[t, j, r].astype(jnp.float32)
                total = total + came[probes:]
                lost = lost + came[:probes]
            plain = sum_blocks(total) + lost
            ag[t, j, core, chip] = jnp.concatenate([plain, total], axis=0).astype(jnp.bfloat16)
            for r in reversed(range(1, chips)):
                send(gather(j, r))
            send(forward(j, 0))

        def add_image(j, which_core, which_chip):
            at = pl.ds(pl.multiple_of(start_of(which_core, j) + which_chip * sub, 128), sub)
            part = lax.dot_general(
                ag[t, j, which_core, which_chip], z[:, at],
                (((1,), (1,)), ((), ())), preferred_element_type=jnp.float32)
            image[group] = image[group] + part

        away_part(0)
        if first_use:
            own_part(0)
            pl.semaphore_wait(barrier, len(peers))
        send_pair(0)
        if not first_use:
            own_part(0)
        yield
        reduce_pair(0)
        yield
        image[group] = jnp.zeros((rows + probes, local), jnp.float32)
        finish_panel(0)
        yield
        add_image(0, core, chip)
        for r in order[:-1]:
            gather(0, r).wait_recv()
            send(forward(0, r))
            add_image(0, core, source(r))
        yield
        for r in [0] + order[:-1]:
            forward(0, r).wait_recv()
            add_image(0, 1 - core, source(r))

        total_snps = cols * snp
        interaction = jnp.zeros((probes, local), jnp.float32)
        for i, tile in enumerate(tiles):
            interaction = interaction + onehot[tile, :] * image[group, (i + 1) * probes:(i + 2) * probes, :]
        interaction = interaction + swap(interaction)
        weighted = var_ref[0] * image[group, :probes, :] / total_snps + var_ref[1] * interaction / total_snps
        z_in[t, here] = jnp.where(packed_upper, weighted[:, :half], weighted[:, half:])

        def other_snp(r):
            return lax.rem(here + jnp.where(here < snp // 2, snp - r, r), snp)

        def over_snps(r, recv):
            return remote(z_in.at[t, here], z_in.at[t, here], zs_s.at[t, r], zs_r.at[t, recv],
                          {"snp": other_snp(r)})

        for r in range(1, snp):
            send(over_snps(r, here))
        yield
        for r in range(1, snp):
            over_snps(r, other_snp(r)).wait_recv()
        total = z_in[t, 0]
        for s in range(1, snp):
            total = total + z_in[t, s]
        turned = swap(total)
        whole = jnp.concatenate(
            [jnp.where(packed_upper, total, turned), jnp.where(packed_upper, turned, total)], axis=1)
        result = whole + var_ref[2] * state[group]
        state[group] = result
        out = first_ref if op == 0 else second_ref
        out[...] = result if group == 0 else jnp.where(upper, out[...], result)

    chains = [chain(0), chain(1)]
    for group in TURNS:
        next(chains[group], None)
    for copy in sent:
        copy.wait_send()


def solution(mesh):
    samp, snp = mesh.shape["samp"], mesh.shape["snp"]

    def per_device(genotypes, probes, env_label, variances):
        local, cols = genotypes.shape
        count = probes.shape[0]
        rows = ENVS * count // 2
        chips, _, stages, sub = plan(samp, cols)
        vmem = pltpu.VMEM
        dma = pltpu.SemaphoreType.DMA
        out = pltpu.VMEM((count, local), jnp.float32)
        anywhere = pl.BlockSpec(memory_space=pl.ANY)
        whole = pl.BlockSpec(memory_space=pltpu.VMEM)
        return pl.pallas_call(
            functools.partial(kernel, samp, snp),
            out_shape=(out, out),
            in_specs=[anywhere, anywhere, anywhere, pl.BlockSpec(memory_space=pltpu.SMEM)],
            out_specs=(whole, whole),
            scratch_shapes=[
                vmem((local, cols), jnp.bfloat16),
                vmem((count, local), jnp.bfloat16),
                vmem((1, local), jnp.int32),
                vmem((2, rows, local), jnp.bfloat16),
                vmem((rows, local), jnp.float32),
                vmem((2, count, local), jnp.float32),
                vmem((2, rows + count, local), jnp.float32),
                vmem((2, chips, rows, sub), jnp.float32),
                vmem((4, stages, chips, rows, sub), jnp.float32),
                vmem((4, stages, chips, rows, sub), jnp.float32),
                vmem((4, stages, chips, rows + count, sub), jnp.bfloat16),
                vmem((4, stages, chips, rows + count, sub), jnp.bfloat16),
                vmem((4, stages, 2, chips, rows + count, sub), jnp.bfloat16),
                vmem((4, snp, count, local // 2), jnp.float32),
                dma((stages, 2)), dma((2,)),
                dma((4, stages, chips)), dma((4, stages, chips)),
                dma((4, stages, chips)), dma((4, stages, chips)),
                dma((4, stages, chips)), dma((4, stages, chips)),
                dma((4, stages, chips)), dma((4, stages, chips)),
                dma((4, snp)), dma((4, snp)),
            ],
            compiler_params=pltpu.CompilerParams(
                collective_id=0, has_side_effects=True, vmem_limit_bytes=56 * 1024 * 1024),
        )(genotypes, probes, env_label.reshape(1, local), variances)

    return jax.shard_map(
        per_device,
        mesh=mesh,
        in_specs=(P("samp", "snp"), P(None, "samp"), P("samp"), P()),
        out_specs=(P(None, "samp"), P(None, "samp")),
        check_vma=False,
    )
```
